512 devices in a mesh: section: 4 (over z_lo), th: 16 (over z_hi, y), tw: 8 (over x, core).
Axes of the slice: x: 4, y: 4, z: 16 (z_hi: 4, z_lo: 4; z = z_hi * 4 + z_lo), core: 2. Of those that a mesh axis runs over, the one named last changes fastest.
Arguments:
- features: bfloat16 [16, 256, 256, 128], P('section', 'th', 'tw'), may hold values from -11 to 11, as said below
- norm_gain: float32 [128], replicated, may hold values from 0.25 to 1.75
- norm_shift: float32 [128], replicated, may hold values from -3 to 3
- first_kernel: bfloat16 [3, 3, 3, 128, 128], replicated, may hold values from -0.109375 to 0.109375
- second_gain: float32 [128], replicated, may hold values from 0.25 to 1.75
- second_shift: float32 [128], replicated, may hold values from -3 to 3
- second_kernel: bfloat16 [3, 3, 3, 128, 128], replicated, may hold values from -0.109375 to 0.109375
Outputs:
- block_out: bfloat16 [16, 256, 256, 128], P('section', 'th', 'tw')
The draws below stay inside these ranges and needn't reach their ends.
Inputs may be any that keep to these rules, and one draw needn't show every extreme that they name: `features`: activations of order one.
All inputs are finite; a program needn't handle non-finite values.
Results may differ from the reference program's by a relative error of at most 0.0038.
Values may be sent and summed in bfloat16 or wider, within the bound.
No kernel may reach another device: no remote copies, remote signals or barrier semaphores. Data moves between devices by JAX's collectives and lax.ppermute only.
A program may use at most 128 MiB of HBM per device.

```python
import jax
import jax.numpy as jnp
from jax import lax

C = 128
GROUPS = 32
FRAMES = 16
HEIGHT = 256
WIDTH = 256


def draw_features(key, part):
    base = jax.random.fold_in(key, 7319)
    key_offset = jax.random.fold_in(base, 0)
    key_noise = jax.random.fold_in(base, 2)
    key_frame = jax.random.fold_in(base, 3)
    key_scale = jax.random.fold_in(base, 4)
    key_row = jax.random.fold_in(base, 5)
    key_col = jax.random.fold_in(base, 6)
    time_frac = jnp.arange(FRAMES, dtype=jnp.float32) / max(FRAMES - 1, 1)
    shape = (FRAMES, HEIGHT, WIDTH, C)
    offset = 0.7 * jax.random.normal(key_offset, (C,), jnp.float32)
    noise = jnp.clip(jax.random.normal(key_noise, shape, jnp.float32), -4.0, 4.0)
    frame_off = 1.0 - 2.0 * time_frac + jax.random.uniform(key_frame, (FRAMES,), jnp.float32, -0.5, 0.5)
    frame_scale = jax.random.uniform(key_scale, (FRAMES,), jnp.float32, 0.4, 1.6)
    row_off = jax.random.uniform(key_row, (HEIGHT,), jnp.float32, 0.4, 1.6)
    col_level = jax.random.uniform(key_col, (WIDTH,), jnp.float32, 0.6, 1.8)
    mean_part = offset[None, None, None, :] * frame_off[:, None, None, None] * row_off[None, :, None, None]
    noise_part = frame_scale[:, None, None, None] * col_level[None, None, :, None] * noise
    return jnp.clip(mean_part + noise_part, -11.0, 11.0).astype(jnp.bfloat16)


def normal_values(stream_key, shape, deviation, reach, kind=jnp.bfloat16):
    drawn = deviation * jax.random.normal(stream_key, shape, jnp.float32)
    return jnp.clip(drawn, min=-reach, max=reach).astype(kind)


def setup_inputs(seed: int = 0) -> dict:
    streams_of = jax.random.split(jax.random.key(seed), 8)
    return {
        "features": draw_features(jax.random.fold_in(streams_of[7], 71), 0),
        "norm_gain": jnp.clip(1.0 + 0.15 * jax.random.normal(streams_of[1], (C,), jnp.float32), 0.25, 1.75),
        "norm_shift": normal_values(streams_of[2], (C,), 0.5, 3.0, jnp.float32),
        "first_kernel": normal_values(streams_of[3], (3, 3, 3, C, C), (27 * C) ** -0.5, 0.109375),
        "second_gain": jnp.clip(1.0 + 0.15 * jax.random.normal(streams_of[4], (C,), jnp.float32), 0.25, 1.75),
        "second_shift": normal_values(streams_of[5], (C,), 0.5, 3.0, jnp.float32),
        "second_kernel": normal_values(streams_of[6], (3, 3, 3, C, C), (27 * C) ** -0.5, 0.109375),
    }


def causal_conv(padded, kernel):
    frames = padded.shape[0] - 2
    rows = padded.shape[1] - 2
    cols = padded.shape[2] - 2
    chans = padded.shape[3]
    stacked = jnp.concatenate([padded[:, :, d:d + cols, :] for d in range(3)], axis=-1)
    taps = kernel.reshape(3, 3, 3 * chans, kernel.shape[-1])
    total = jnp.zeros((frames * rows * cols, kernel.shape[-1]), jnp.float32)
    for dt in range(3):
        for dh in range(3):
            window = stacked[dt:dt + frames, dh:dh + rows].reshape(-1, 3 * chans)
            total = total + jnp.dot(window, taps[dt, dh], preferred_element_type=jnp.float32)
    return total.reshape(frames, rows, cols, kernel.shape[-1])

def group_norm_act(values, gain, shift):
    chans = values.shape[-1]
    grouped = values.astype(jnp.float32).reshape(-1, GROUPS, chans // GROUPS)
    mean = lax.optimization_barrier(jnp.mean(grouped, axis=(0, 2), keepdims=True))
    var = lax.optimization_barrier(jnp.mean((grouped - mean) ** 2, axis=(0, 2), keepdims=True))
    normed = ((grouped - mean) / jnp.sqrt(var + 1e-06)).reshape(values.shape) * gain + shift
    return jax.nn.silu(normed).astype(jnp.bfloat16)

def pad_clip(values):
    return jnp.pad(values, ((2, 0), (1, 1), (1, 1), (0, 0)))

def reference(features, norm_gain, norm_shift, first_kernel, second_gain, second_shift, second_kernel):
    first_act = group_norm_act(features, norm_gain, norm_shift)
    hidden = causal_conv(pad_clip(first_act), first_kernel)
    second_act = group_norm_act(hidden, second_gain, second_shift)
    branch = causal_conv(pad_clip(second_act), second_kernel)
    return (features.astype(jnp.float32) + branch).astype(jnp.bfloat16)
```

```python
import jax
import jax.numpy as jnp
from jax import lax
from jax.sharding import Mesh
from jax.sharding import PartitionSpec as P

GROUPS = 32
TH = ("th_0", "th_1")
TW = ("tw_0", "tw_1")


def gathered_sum(value, axis):
    return jnp.sum(lax.all_gather(value, axis), axis=0)


def shifted(value, axis, step):
    count = lax.axis_size(axis)
    pairs = [(i, i + step) for i in range(count) if 0 <= i + step < count]
    return lax.ppermute(value, axis, pairs)


def extended_and_summed(block, sums):
    before = shifted(block[-2:], "section", 1)
    sums = gathered_sum(sums, "th_0")
    before, sums = lax.optimization_barrier((before, sums))
    left = shifted(jnp.concatenate([before[:, :, -1:], block[:, :, -1:]], 0), TW, 1)
    right = shifted(jnp.concatenate([before[:, :, :1], block[:, :, :1]], 0), TW, -1)
    sums = gathered_sum(gathered_sum(sums, "tw_0"), "tw_1")
    left, right, sums = lax.optimization_barrier((left, right, sums))
    wide = jnp.concatenate([left, jnp.concatenate([before, block], 0), right], 2)
    above = shifted(wide[:, -1:], TH, 1)
    below = shifted(wide[:, :1], TH, -1)
    sums = gathered_sum(gathered_sum(sums, "th_1"), "section")
    above, below, sums = lax.optimization_barrier((above, below, sums))
    return jnp.concatenate([above, wide, below], 1), sums


def inside(shape):
    frame = lax.broadcasted_iota(jnp.int32, shape, 0) + 4 * lax.axis_index("section")
    row = lax.broadcasted_iota(jnp.int32, shape, 1) + 16 * lax.axis_index(TH)
    col = lax.broadcasted_iota(jnp.int32, shape, 2) + 32 * lax.axis_index(TW)
    return (frame >= 2) & (row >= 1) & (row <= 256) & (col >= 1) & (col <= 256)


def local_sums(values):
    flat = values.reshape(-1, values.shape[-1])
    return jnp.concatenate([jnp.sum(flat, 0), jnp.sum(flat * flat, 0)])[None]


def scale_and_offset(sums, count, gain, shift):
    per = sums.shape[-1] // 2 // GROUPS
    totals = jnp.sum(sums.reshape(2, GROUPS, per), -1) / count
    mean = jnp.repeat(totals[0], per)
    var = jnp.repeat(totals[1] - totals[0] * totals[0], per)
    scale = gain / jnp.sqrt(var + 1e-06)
    return scale, shift - mean * scale


def activated(block, own, gain, shift):
    count = own.size // GROUPS * 512
    full, sums = extended_and_summed(block, local_sums(own))
    scale, offset = scale_and_offset(sums, count, gain, shift)
    act = jax.nn.silu(full.astype(jnp.float32) * scale + offset)
    return jnp.where(inside(full.shape[:3] + (1,)), act, 0).astype(jnp.bfloat16)


def causal_conv(padded, kernel):
    frames = padded.shape[0] - 2
    rows = padded.shape[1] - 2
    cols = padded.shape[2] - 2
    chans = padded.shape[3]
    stacked = jnp.concatenate([padded[:, :, d : d + cols, :] for d in range(3)], axis=-1)
    taps = kernel.reshape(3, 3, 3 * chans, kernel.shape[-1])
    total = jnp.zeros((frames * rows * cols, kernel.shape[-1]), jnp.float32)
    for dt in range(3):
        for dh in range(3):
            window = stacked[dt : dt + frames, dh : dh + rows].reshape(-1, 3 * chans)
            total = total + jnp.dot(window, taps[dt, dh], preferred_element_type=jnp.float32)
    return total.reshape(frames, rows, cols, kernel.shape[-1])


def shards(features, norm_gain, norm_shift, first_kernel, second_gain, second_shift, second_kernel):
    inputs = features.astype(jnp.float32)
    first_act = activated(features, inputs, norm_gain, norm_shift)
    hidden = causal_conv(first_act, first_kernel)
    second_act = activated(hidden.astype(jnp.bfloat16), hidden, second_gain, second_shift)
    branch = causal_conv(second_act, second_kernel)
    return (inputs + branch).astype(jnp.bfloat16)


def solution(mesh):
    torus = Mesh(
        mesh.devices.reshape(mesh.shape["section"], 4, 4, 4, 2),
        ("section", "th_0", "th_1", "tw_0", "tw_1"),
    )
    return jax.shard_map(
        shards,
        mesh=torus,
        in_specs=(P("section", TH, TW, None), P(), P(), P(), P(), P(), P()),
        out_specs=P("section", TH, TW, None),
        check_vma=False,
    )
```

```python
import functools

import jax
import jax.numpy as jnp
from jax import lax
from jax.experimental import pallas as pl
from jax.experimental.pallas import tpu as pltpu
from jax.sharding import Mesh
from jax.sharding import PartitionSpec as P

TH = ("th_0", "th_1")
TW = ("tw_0", "tw_1")
PER = 4
CHUNK = 8
EPS = 1e-06
VMEM = 20 * 2**20
F32 = jnp.float32
BF16 = jnp.bfloat16


def gathered_sum(value, axis):
    return jnp.sum(lax.all_gather(value, axis), axis=0)


def shifted(value, axis, step):
    count = lax.axis_size(axis)
    pairs = [(i, i + step) for i in range(count) if 0 <= i + step < count]
    return lax.ppermute(value, axis, pairs)


def scale_and_offset(sums_ref, gain_ref, shift_ref, count):
    totals = jnp.sum(sums_ref[...], axis=0)
    lane = lax.broadcasted_iota(jnp.int32, totals.shape, 1)
    for width in (1, 2):
        back = pltpu.roll(totals, width, 1)
        ahead = pltpu.roll(totals, totals.shape[1] - width, 1)
        totals = totals + jnp.where(lane // width % 2 == 0, ahead, back)
    totals = totals * (1.0 / count)
    mean = totals[0:1]
    var = totals[1:2] - mean * mean
    scale = gain_ref[...] / jnp.sqrt(var + EPS)
    return 0.5 * scale, 0.5 * (shift_ref[...] - mean * scale)


def silu_of_double(half):
    return half + half * jnp.tanh(half)


def edges():
    th = lax.axis_index("th_0") * lax.axis_size("th_1") + lax.axis_index("th_1")
    tw = lax.axis_index("tw_0") * lax.axis_size("tw_1") + lax.axis_index("tw_1")
    section = lax.axis_index("section")
    last_th = lax.axis_size(TH) - 1
    last_tw = lax.axis_size(TW) - 1
    tests = (section > 0, th > 0, th < last_th, tw > 0, tw < last_tw)
    return [jnp.where(t, 1.0, 0.0).astype(F32) for t in tests]


def store_act(act_ref, h, m, pairs, row_ok, before_ok, column_ok):
    ok = row_ok if column_ok is None else row_ok * column_ok
    pairs = [pairs[0] * (ok * before_ok), pairs[1] * ok, pairs[2] * ok]
    low = lax.broadcasted_iota(jnp.int32, pairs[0].shape, 0) < 4
    mid = [pltpu.roll(jnp.where(low, b, a), 4, 0) for a, b in zip(pairs[:2], pairs[1:])]
    for dt, halves in enumerate((pairs[:2], mid, pairs[1:])):
        act_ref[dt, h, m] = jnp.concatenate(halves, 0).astype(BF16)


def column_masks(left_ok, right_ok):
    chunk = lax.broadcasted_iota(jnp.int32, (8, 128), 0) % 4
    return jnp.where(chunk == 0, left_ok, 1.0), jnp.where(chunk == 3, right_ok, 1.0)


def conv_block(act_ref, kernel_ref, acc_ref, start, rows, cols):
    size = rows * cols * 16
    taps = [(dt, di, dj) for dt in range(3) for di in range(3) for dj in range(3)]
    step = 2
    for k in range(0, 27, step):
        part = taps[k : k + step]
        lhs = jnp.concatenate(
            [
                act_ref[dt, pl.ds(start + di, rows), dj : dj + cols].reshape(size, 128)
                for dt, di, dj in part
            ],
            axis=1,
        )
        rhs = kernel_ref[k * 128 : (k + len(part)) * 128, :]
        new = jnp.dot(lhs, rhs, preferred_element_type=F32)
        acc_ref[...] = new if k == 0 else acc_ref[...] + new


def prepare_body(feat_ref, last_ref, top_ref, bottom_ref, head_ref, tail_ref, sums_ref):
    last_ref[...] = feat_ref[2:4]
    top_ref[...] = feat_ref[:, 0:2]
    bottom_ref[...] = feat_ref[:, 14:16]
    head_ref[...] = feat_ref[:, :, 0:2]
    tail_ref[...] = feat_ref[:, :, 30:32]
    first = jnp.zeros((8, 128), F32)
    second = jnp.zeros((8, 128), F32)
    for t in range(4):
        for h in range(0, 16, 4):
            part = feat_ref[t, h : h + 4].astype(F32).reshape(16, 8, 128)
            first += jnp.sum(part, 0)
            second += jnp.sum(part * part, 0)
    sums_ref[0:1, :] = jnp.sum(first, 0, keepdims=True)
    sums_ref[1:2, :] = jnp.sum(second, 0, keepdims=True)


ROWS1, COLS1, BLOCK1 = 18, CHUNK + 2, 6
ROWS2, COLS2, BLOCK2 = 16, CHUNK, 8


def first_body(count, feat_ref, before_ref, above_ref, below_ref, left_ref, right_ref, sums_ref,
               gain_ref, shift_ref, kernel_ref, hidden_ref, halo_ref, out_sums_ref,
               flat_ref, act_ref, acc_ref, taps_ref, taps_sem):
    fetch = pltpu.make_async_copy(kernel_ref, taps_ref, taps_sem)
    fetch.start()
    scale, offset = scale_and_offset(sums_ref, gain_ref, shift_ref, count)
    before_ok, above_ok, below_ok, left_ok, right_ok = edges()
    left_mask, right_mask = column_masks(left_ok, right_ok)

    flat_ref[2:6, 2:18, 8:40] = feat_ref[...].astype(F32)
    flat_ref[0:2, 2:18, 8:40] = before_ref[...].astype(F32)
    flat_ref[:, 0:2, 8:40] = above_ref[...].astype(F32)
    flat_ref[:, 18:20, 8:40] = below_ref[...].astype(F32)
    flat_ref[:, :, 6:8] = left_ref[...].astype(F32)
    flat_ref[:, :, 40:42] = right_ref[...].astype(F32)

    def fill(h, _):
        row_ok = jnp.where(h < 2, above_ok, jnp.where(h >= 18, below_ok, 1.0))
        for m in range(COLS1 + 2):
            pairs = []
            for t in (0, 2, 4):
                raw = jnp.concatenate(
                    [flat_ref[t + i, h, pl.ds(6 + m, 4, stride=8), :] for i in range(2)], 0
                )
                pairs.append(silu_of_double(raw * scale + offset))
            column_ok = left_mask if m < 2 else right_mask if m >= COLS1 else None
            store_act(act_ref, h, m, pairs, row_ok, before_ok, column_ok)
        return 0

    lax.fori_loop(0, ROWS1 + 2, fill, 0)

    fetch.wait()

    def conv(b, _):
        conv_block(act_ref, taps_ref, acc_ref, b * BLOCK1, BLOCK1, COLS1)
        hidden_ref[pl.ds(b * BLOCK1, BLOCK1)] = acc_ref[...].reshape(BLOCK1, COLS1, 16, 128)
        return 0

    lax.fori_loop(0, ROWS1 // BLOCK1, conv, 0)

    def total(h, carry):
        own = hidden_ref[h, 1 : CHUNK + 1].reshape(CHUNK * 2, 8, 128)
        return carry[0] + jnp.sum(own, 0), carry[1] + jnp.sum(own * own, 0)

    zero = jnp.zeros((8, 128), F32)
    first, second = lax.fori_loop(1, ROWS1 - 1, total, (zero, zero))
    out_sums_ref[0:1, :] = jnp.sum(first, 0, keepdims=True)
    out_sums_ref[1:2, :] = jnp.sum(second, 0, keepdims=True)

    def last_frames(h, _):
        for j in range(COLS1 // 2):
            both = [hidden_ref[h, 2 * j + i, 8:16, :] for i in range(2)]
            halo_ref[h, j] = jnp.concatenate(both, 0).astype(BF16)
        return 0

    lax.fori_loop(0, ROWS1, last_frames, 0)


def second_body(count, hidden_ref, halo_ref, sums_ref, gain_ref, shift_ref, kernel_ref, feat_ref,
                out_ref, act_ref, acc_ref, flat_ref):
    scale, offset = scale_and_offset(sums_ref, gain_ref, shift_ref, count)
    before_ok, above_ok, below_ok, left_ok, right_ok = edges()
    left_mask, right_mask = column_masks(left_ok, right_ok)

    def fill(h, _):
        row_ok = jnp.where(h < 1, above_ok, jnp.where(h >= 17, below_ok, 1.0))
        for m in range(COLS2 + 2):
            halo = halo_ref[h, m // 2].astype(F32)[m % 2 * 8 : m % 2 * 8 + 8]
            raws = (halo, hidden_ref[h, m, 0:8, :], hidden_ref[h, m, 8:16, :])
            pairs = [silu_of_double(raw * scale + offset) for raw in raws]
            column_ok = left_mask if m < 1 else right_mask if m > COLS2 else None
            store_act(act_ref, h, m, pairs, row_ok, before_ok, column_ok)
        return 0

    lax.fori_loop(0, ROWS2 + 2, fill, 0)

    def conv(b, _):
        conv_block(act_ref, kernel_ref, acc_ref, b * BLOCK2, BLOCK2, COLS2)

        def spread(i, _):
            h = b * BLOCK2 + i
            for m in range(COLS2):
                tile = acc_ref[pl.ds(pl.multiple_of((i * COLS2 + m) * 16, 16), 16), :]
                for t in range(4):
                    flat_ref[t, pl.ds(m, 4, stride=8), :] = tile[4 * t : 4 * t + 4]
            for t in range(4):
                total = feat_ref[t, h].astype(F32) + flat_ref[t]
                out_ref[t, h] = total.astype(BF16)
            return 0

        lax.fori_loop(0, BLOCK2, spread, 0)
        return 0

    lax.fori_loop(0, ROWS2 // BLOCK2, conv, 0)


def in_vmem(count):
    return [pl.BlockSpec(memory_space=pltpu.VMEM)] * count


def shards(features, norm_gain, norm_shift, first_kernel, second_gain, second_shift, second_kernel):
    count = features.size // features.shape[-1] * PER
    for axis in ("section", *TH, *TW):
        count *= lax.axis_size(axis)
    last, top, bottom, head, tail, sums = pl.pallas_call(
        prepare_body,
        out_shape=tuple(
            jax.ShapeDtypeStruct(shape, BF16)
            for shape in (
                (2, 16, 32, 128), (4, 2, 32, 128), (4, 2, 32, 128), (4, 16, 2, 128), (4, 16, 2, 128)
            )
        ) + (jax.ShapeDtypeStruct((2, 128), F32),),
        in_specs=in_vmem(1),
        out_specs=tuple(in_vmem(6)),
        compiler_params=pltpu.CompilerParams(vmem_limit_bytes=VMEM),
        name="prepare",
    )(features)

    before = shifted(last, "section", 1)
    sums = gathered_sum(sums, TW)
    before, sums = lax.optimization_barrier((before, sums))
    above = shifted(jnp.concatenate([before[:, -2:], bottom], 0), TH, 1)
    below = shifted(jnp.concatenate([before[:, :2], top], 0), TH, -1)
    sums = gathered_sum(sums, "th_1")
    sums = gathered_sum(sums, "section")
    above, below, sums = lax.optimization_barrier((above, below, sums))

    def columns(own, s):
        own = jnp.concatenate([before[:, :, s], own], 0)
        return jnp.concatenate([above[:, :, s], own, below[:, :, s]], 1)

    left = shifted(columns(tail, slice(-2, None)), TW, 1)
    right = shifted(columns(head, slice(0, 2)), TW, -1)
    sums = lax.all_gather(sums, "th_0")

    hidden, halo, sums = pl.pallas_call(
        functools.partial(first_body, count),
        out_shape=(
            jax.ShapeDtypeStruct((ROWS1, COLS1, 16, 128), F32),
            jax.ShapeDtypeStruct((ROWS1, COLS1 // 2, 16, 128), BF16),
            jax.ShapeDtypeStruct((2, 128), F32),
        ),
        in_specs=[*in_vmem(9), pl.BlockSpec(memory_space=pltpu.HBM)],
        out_specs=tuple(in_vmem(3)),
        scratch_shapes=[
            pltpu.VMEM((6, 20, 48, 128), F32),
            pltpu.VMEM((3, ROWS1 + 2, COLS1 + 2, 16, 128), BF16),
            pltpu.VMEM((BLOCK1 * COLS1 * 16, 128), F32),
            pltpu.VMEM((27 * 128, 128), BF16),
            pltpu.SemaphoreType.DMA,
        ],
        compiler_params=pltpu.CompilerParams(vmem_limit_bytes=VMEM),
        name="first_conv",
    )(features, before, above, below, left, right, sums, norm_gain[None], norm_shift[None],
      pltpu.with_memory_space_constraint(first_kernel.reshape(-1, 128), pltpu.HBM))

    halo = shifted(halo, "section", 1)
    for axis in (TW, "th_1", "section"):
        sums = gathered_sum(sums, axis)
    sums = lax.all_gather(sums, "th_0")

    return pl.pallas_call(
        functools.partial(second_body, count),
        out_shape=jax.ShapeDtypeStruct(features.shape, BF16),
        in_specs=in_vmem(7),
        out_specs=in_vmem(1)[0],
        scratch_shapes=[
            pltpu.VMEM((3, ROWS2 + 2, COLS2 + 2, 16, 128), BF16),
            pltpu.VMEM((BLOCK2 * COLS2 * 16, 128), F32),
            pltpu.VMEM((4, 32, 128), F32),
        ],
        compiler_params=pltpu.CompilerParams(vmem_limit_bytes=VMEM),
        name="second_conv",
    )(hidden, halo, sums, second_gain[None], second_shift[None], second_kernel.reshape(-1, 128), features)


def solution(mesh):
    torus = Mesh(
        mesh.devices.reshape(mesh.shape["section"], 4, 4, 4, 2),
        ("section", "th_0", "th_1", "tw_0", "tw_1"),
    )
    return jax.shard_map(
        shards,
        mesh=torus,
        in_specs=(P("section", TH, TW, None), P(), P(), P(), P(), P(), P()),
        out_specs=P("section", TH, TW, None),
        check_vma=False,
    )
```

```python
import functools

import jax
import jax.numpy as jnp
from jax import lax
from jax.experimental import pallas as pl
from jax.experimental.pallas import tpu as pltpu
from jax.sharding import Mesh
from jax.sharding import PartitionSpec as P

TH = ("th_0", "th_1")
TW = ("tw_0", "tw_1")
PER = 4
CHUNK = 8
EPS = 1e-06
VMEM = 20 * 2**20
F32 = jnp.float32
BF16 = jnp.bfloat16


def gathered_sum(value, axis):
    return jnp.sum(lax.all_gather(value, axis), axis=0)


def shifted(value, axis, step):
    count = lax.axis_size(axis)
    pairs = [(i, i + step) for i in range(count) if 0 <= i + step < count]
    return lax.ppermute(value, axis, pairs)


def swapped(toward_next, toward_last, axis, odd):
    count = lax.axis_size(axis)

    def swap(value, first):
        pairs = [(i, i + 1) for i in range(first, count - 1, 2)]
        return lax.ppermute(value, axis, pairs + [(b, a) for a, b in pairs])

    even_first = swap(jnp.where(odd, toward_last, toward_next), 0)
    odd_first = swap(jnp.where(odd, toward_next, toward_last), 1)
    return jnp.where(odd, even_first, odd_first), jnp.where(odd, odd_first, even_first)


def scale_and_offset(sums_ref, gain_ref, shift_ref, count):
    totals = jnp.sum(sums_ref[...], axis=0)
    lane = lax.broadcasted_iota(jnp.int32, totals.shape, 1)
    for width in (1, 2):
        back = pltpu.roll(totals, width, 1)
        ahead = pltpu.roll(totals, totals.shape[1] - width, 1)
        totals = totals + jnp.where(lane // width % 2 == 0, ahead, back)
    totals = totals * (1.0 / count)
    mean = totals[0:1]
    var = totals[1:2] - mean * mean
    scale = gain_ref[...] / jnp.sqrt(var + EPS)
    return 0.5 * scale, 0.5 * (shift_ref[...] - mean * scale)


def silu_of_double(half):
    return half + half * jnp.tanh(half)


def edges():
    th = lax.axis_index("th_0") * lax.axis_size("th_1") + lax.axis_index("th_1")
    tw = lax.axis_index("tw_0") * lax.axis_size("tw_1") + lax.axis_index("tw_1")
    section = lax.axis_index("section")
    last_th = lax.axis_size(TH) - 1
    last_tw = lax.axis_size(TW) - 1
    tests = (section > 0, th > 0, th < last_th, tw > 0, tw < last_tw)
    return [jnp.where(t, 1.0, 0.0).astype(F32) for t in tests]


def store_act(act_ref, h, m, pairs, row_ok, before_ok, column_ok):
    ok = row_ok if column_ok is None else row_ok * column_ok
    pairs = [pairs[0] * (ok * before_ok), pairs[1] * ok, pairs[2] * ok]
    low = lax.broadcasted_iota(jnp.int32, pairs[0].shape, 0) < 4
    mid = [pltpu.roll(jnp.where(low, b, a), 4, 0) for a, b in zip(pairs[:2], pairs[1:])]
    for dt, halves in enumerate((pairs[:2], mid, pairs[1:])):
        act_ref[dt, h, m] = jnp.concatenate(halves, 0).astype(BF16)


def column_masks(left_ok, right_ok):
    chunk = lax.broadcasted_iota(jnp.int32, (8, 128), 0) % 4
    return jnp.where(chunk == 0, left_ok, 1.0), jnp.where(chunk == 3, right_ok, 1.0)


def conv_block(act_ref, kernel_ref, pair_ref, single_ref, start, rows, cols):
    slabs = [(dt, di) for dt in range(3) for di in range(3)]

    def lhs(parts, width):
        parts = [act_ref[dt, pl.ds(start + di, rows), dj : dj + width] for dt, di, dj in parts]
        return jnp.concatenate([p.reshape(rows * width * 16, 128) for p in parts], 1)

    def tap(dt, di, dj):
        k = ((dt * 3 + di) * 3 + dj) * 128
        return kernel_ref[k : k + 128, :]

    def wide(slab):
        return jnp.concatenate([tap(*slab, 0), tap(*slab, 1)], 1)

    for k in range(0, 9, 2):
        first = slabs[k]
        if k < 8:
            left = lhs([(*first, 0), (*slabs[k + 1], 0)], cols + 1)
            right = jnp.concatenate([wide(first), wide(slabs[k + 1])], 0)
        else:
            left = lhs([(*first, 0), (*first, 2)], cols + 1)
            last = tap(*first, 2)
            last = jnp.concatenate([last, jnp.zeros_like(last)], 1)
            right = jnp.concatenate([wide(first), last], 0)
        new = jnp.dot(left, right, preferred_element_type=F32)
        pair_ref[...] = new if k == 0 else pair_ref[...] + new
    for k in range(0, 8, 2):
        left = lhs([(*slabs[k], 2), (*slabs[k + 1], 2)], cols)
        right = jnp.concatenate([tap(*slabs[k], 2), tap(*slabs[k + 1], 2)], 0)
        new = jnp.dot(left, right, preferred_element_type=F32)
        single_ref[...] = new if k == 0 else single_ref[...] + new


def clear_last_column(act_ref, rows, column):
    for h in range(rows):
        act_ref[2, h, column] = jnp.zeros((16, 128), BF16)


def prepare_body(feat_ref, last_ref, top_ref, bottom_ref, head_ref, tail_ref, sums_ref):
    last_ref[...] = feat_ref[2:4]
    top_ref[...] = feat_ref[:, 0:2]
    bottom_ref[...] = feat_ref[:, 14:16]
    head_ref[...] = feat_ref[:, :, 0:2]
    tail_ref[...] = feat_ref[:, :, 30:32]
    first = jnp.zeros((8, 128), F32)
    second = jnp.zeros((8, 128), F32)
    for t in range(4):
        for h in range(0, 16, 4):
            part = feat_ref[t, h : h + 4].astype(F32).reshape(16, 8, 128)
            first += jnp.sum(part, 0)
            second += jnp.sum(part * part, 0)
    sums_ref[0:1, :] = jnp.sum(first, 0, keepdims=True)
    sums_ref[1:2, :] = jnp.sum(second, 0, keepdims=True)


ROWS1, COLS1, BLOCK1 = 18, CHUNK + 2, 6
ROWS2, COLS2, BLOCK2 = 16, CHUNK, 8


def first_body(count, feat_ref, before_ref, above_ref, below_ref, left_ref, right_ref, sums_ref,
               gain_ref, shift_ref, kernel_ref, hidden_ref, halo_ref, out_sums_ref,
               flat_ref, act_ref, pair_ref, single_ref, taps_ref, taps_sem):
    fetch = pltpu.make_async_copy(kernel_ref, taps_ref, taps_sem)
    fetch.start()
    scale, offset = scale_and_offset(sums_ref, gain_ref, shift_ref, count)
    before_ok, above_ok, below_ok, left_ok, right_ok = edges()
    left_mask, right_mask = column_masks(left_ok, right_ok)

    flat_ref[2:6, 2:18, 8:40] = feat_ref[...].astype(F32)
    flat_ref[0:2, 2:18, 8:40] = before_ref[...].astype(F32)
    flat_ref[:, 0:2, 8:40] = above_ref[...].astype(F32)
    flat_ref[:, 18:20, 8:40] = below_ref[...].astype(F32)
    flat_ref[:, :, 6:8] = left_ref[...].astype(F32)
    flat_ref[:, :, 40:42] = right_ref[...].astype(F32)

    def fill(h, _):
        row_ok = jnp.where(h < 2, above_ok, jnp.where(h >= 18, below_ok, 1.0))
        for m in range(COLS1 + 2):
            pairs = []
            for t in (0, 2, 4):
                raw = jnp.concatenate(
                    [flat_ref[t + i, h, pl.ds(6 + m, 4, stride=8), :] for i in range(2)], 0
                )
                pairs.append(silu_of_double(raw * scale + offset))
            column_ok = left_mask if m < 2 else right_mask if m >= COLS1 else None
            store_act(act_ref, h, m, pairs, row_ok, before_ok, column_ok)
        return 0

    lax.fori_loop(0, ROWS1 + 2, fill, 0)

    clear_last_column(act_ref, ROWS1 + 2, COLS1 + 2)
    fetch.wait()

    def conv(b, _):
        conv_block(act_ref, taps_ref, pair_ref, single_ref, b * BLOCK1, BLOCK1, COLS1)
        both = pair_ref[...].reshape(BLOCK1, COLS1 + 1, 16, 256)
        total = both[:, :COLS1, :, :128] + both[:, 1:, :, 128:]
        total += single_ref[...].reshape(BLOCK1, COLS1, 16, 128)
        hidden_ref[pl.ds(b * BLOCK1, BLOCK1)] = total
        return 0

    lax.fori_loop(0, ROWS1 // BLOCK1, conv, 0)

    def total(h, carry):
        own = hidden_ref[h, 1 : CHUNK + 1].reshape(CHUNK * 2, 8, 128)
        return carry[0] + jnp.sum(own, 0), carry[1] + jnp.sum(own * own, 0)

    zero = jnp.zeros((8, 128), F32)
    first, second = lax.fori_loop(1, ROWS1 - 1, total, (zero, zero))
    out_sums_ref[0:1, :] = jnp.sum(first, 0, keepdims=True)
    out_sums_ref[1:2, :] = jnp.sum(second, 0, keepdims=True)

    def last_frames(h, _):
        for j in range(COLS1 // 2):
            both = [hidden_ref[h, 2 * j + i, 8:16, :] for i in range(2)]
            halo_ref[h, j] = jnp.concatenate(both, 0).astype(BF16)
        return 0

    lax.fori_loop(0, ROWS1, last_frames, 0)


def second_body(count, hidden_ref, halo_ref, sums_ref, gain_ref, shift_ref, kernel_ref, feat_ref,
                out_ref, act_ref, pair_ref, single_ref, flat_ref):
    scale, offset = scale_and_offset(sums_ref, gain_ref, shift_ref, count)
    before_ok, above_ok, below_ok, left_ok, right_ok = edges()
    left_mask, right_mask = column_masks(left_ok, right_ok)

    def fill(h, _):
        row_ok = jnp.where(h < 1, above_ok, jnp.where(h >= 17, below_ok, 1.0))
        for m in range(COLS2 + 2):
            halo = halo_ref[h, m // 2].astype(F32)[m % 2 * 8 : m % 2 * 8 + 8]
            raws = (halo, hidden_ref[h, m, 0:8, :], hidden_ref[h, m, 8:16, :])
            pairs = [silu_of_double(raw * scale + offset) for raw in raws]
            column_ok = left_mask if m < 1 else right_mask if m > COLS2 else None
            store_act(act_ref, h, m, pairs, row_ok, before_ok, column_ok)
        return 0

    lax.fori_loop(0, ROWS2 + 2, fill, 0)

    clear_last_column(act_ref, ROWS2 + 2, COLS2 + 2)

    def conv(b, _):
        conv_block(act_ref, kernel_ref, pair_ref, single_ref, b * BLOCK2, BLOCK2, COLS2)

        def spread(i, _):
            h = b * BLOCK2 + i
            for m in range(COLS2):
                at = pl.multiple_of((i * (COLS2 + 1) + m) * 16, 16)
                tile = pair_ref[pl.ds(at, 16), :128] + pair_ref[pl.ds(at + 16, 16), 128:]
                at = pl.multiple_of((i * COLS2 + m) * 16, 16)
                tile += single_ref[pl.ds(at, 16), :]
                for t in range(4):
                    flat_ref[t, pl.ds(m, 4, stride=8), :] = tile[4 * t : 4 * t + 4]
            for t in range(4):
                total = feat_ref[t, h].astype(F32) + flat_ref[t]
                out_ref[t, h] = total.astype(BF16)
            return 0

        lax.fori_loop(0, BLOCK2, spread, 0)
        return 0

    lax.fori_loop(0, ROWS2 // BLOCK2, conv, 0)


def in_vmem(count):
    return [pl.BlockSpec(memory_space=pltpu.VMEM)] * count


def shards(features, norm_gain, norm_shift, first_kernel, second_gain, second_shift, second_kernel):
    count = features.size // features.shape[-1] * PER
    for axis in ("section", *TH, *TW):
        count *= lax.axis_size(axis)
    last, top, bottom, head, tail, sums = pl.pallas_call(
        prepare_body,
        out_shape=tuple(
            jax.ShapeDtypeStruct(shape, BF16)
            for shape in (
                (2, 16, 32, 128), (4, 2, 32, 128), (4, 2, 32, 128), (4, 16, 2, 128), (4, 16, 2, 128)
            )
        ) + (jax.ShapeDtypeStruct((2, 128), F32),),
        in_specs=in_vmem(1),
        out_specs=tuple(in_vmem(6)),
        compiler_params=pltpu.CompilerParams(vmem_limit_bytes=VMEM),
        name="prepare",
    )(features)

    before = shifted(last, "section", 1)
    sums = gathered_sum(sums, TW)
    before, sums = lax.optimization_barrier((before, sums))
    above, below = swapped(
        jnp.concatenate([before[:, -2:], bottom], 0),
        jnp.concatenate([before[:, :2], top], 0),
        TH,
        (lax.axis_index("th_1") & 1) == 1,
    )
    sums = gathered_sum(sums, "th_1")
    sums = gathered_sum(sums, "section")
    above, below, sums = lax.optimization_barrier((above, below, sums))

    def columns(own, s):
        own = jnp.concatenate([before[:, :, s], own], 0)
        return jnp.concatenate([above[:, :, s], own, below[:, :, s]], 1)

    left, right = swapped(
        columns(tail, slice(-2, None)),
        columns(head, slice(0, 2)),
        TW,
        lax.axis_index("tw_1") == 1,
    )
    sums = lax.all_gather(sums, "th_0")

    hidden, halo, sums = pl.pallas_call(
        functools.partial(first_body, count),
        out_shape=(
            jax.ShapeDtypeStruct((ROWS1, COLS1, 16, 128), F32),
            pltpu.VMEM((ROWS1, COLS1 // 2, 16, 128), BF16),
            jax.ShapeDtypeStruct((2, 128), F32),
        ),
        in_specs=[*in_vmem(9), pl.BlockSpec(memory_space=pltpu.HBM)],
        out_specs=tuple(in_vmem(3)),
        scratch_shapes=[
            pltpu.VMEM((6, 20, 48, 128), F32),
            pltpu.VMEM((3, ROWS1 + 2, COLS1 + 3, 16, 128), BF16),
            pltpu.VMEM((BLOCK1 * (COLS1 + 1) * 16, 256), F32),
            pltpu.VMEM((BLOCK1 * COLS1 * 16, 128), F32),
            pltpu.VMEM((27 * 128, 128), BF16),
            pltpu.SemaphoreType.DMA,
        ],
        compiler_params=pltpu.CompilerParams(vmem_limit_bytes=VMEM),
        name="first_conv",
    )(features, before, above, below, left, right, sums, norm_gain[None], norm_shift[None],
      pltpu.with_memory_space_constraint(first_kernel.reshape(-1, 128), pltpu.HBM))

    halo = shifted(halo, "section", 1)
    for axis in (TW, "th_1", "section"):
        sums = gathered_sum(sums, axis)
    sums = lax.all_gather(sums, "th_0")

    return pl.pallas_call(
        functools.partial(second_body, count),
        out_shape=jax.ShapeDtypeStruct(features.shape, BF16),
        in_specs=in_vmem(7),
        out_specs=in_vmem(1)[0],
        scratch_shapes=[
            pltpu.VMEM((3, ROWS2 + 2, COLS2 + 3, 16, 128), BF16),
            pltpu.VMEM((BLOCK2 * (COLS2 + 1) * 16, 256), F32),
            pltpu.VMEM((BLOCK2 * COLS2 * 16, 128), F32),
            pltpu.VMEM((4, 32, 128), F32),
        ],
        compiler_params=pltpu.CompilerParams(vmem_limit_bytes=VMEM),
        name="second_conv",
    )(hidden, halo, sums, second_gain[None], second_shift[None], second_kernel.reshape(-1, 128), features)


def solution(mesh):
    torus = Mesh(
        mesh.devices.reshape(mesh.shape["section"], 4, 4, 4, 2),
        ("section", "th_0", "th_1", "tw_0", "tw_1"),
    )
    return jax.shard_map(
        shards,
        mesh=torus,
        in_specs=(P("section", TH, TW, None), P(), P(), P(), P(), P(), P()),
        out_specs=P("section", TH, TW, None),
        check_vma=False,
    )
```

```python
import functools

import jax
import jax.numpy as jnp
from jax import lax
from jax.experimental import pallas as pl
from jax.experimental.pallas import tpu as pltpu
from jax.sharding import Mesh
from jax.sharding import PartitionSpec as P

TH = ("th_0", "th_1")
TW = ("tw_0", "tw_1")
PER = 4
CHUNK = 8
EPS = 1e-06
VMEM = 20 * 2**20
F32 = jnp.float32
BF16 = jnp.bfloat16


def gathered_sum(value, axis):
    return jnp.sum(lax.all_gather(value, axis), axis=0)


def shifted(value, axis, step):
    count = lax.axis_size(axis)
    pairs = [(i, i + step) for i in range(count) if 0 <= i + step < count]
    return lax.ppermute(value, axis, pairs)


def swapped(toward_next, toward_last, axis, odd):
    count = lax.axis_size(axis)

    def swap(value, first):
        pairs = [(i, i + 1) for i in range(first, count - 1, 2)]
        return lax.ppermute(value, axis, pairs + [(b, a) for a, b in pairs])

    even_first = swap(jnp.where(odd, toward_last, toward_next), 0)
    odd_first = swap(jnp.where(odd, toward_next, toward_last), 1)
    return jnp.where(odd, even_first, odd_first), jnp.where(odd, odd_first, even_first)


def scale_and_offset(sums_ref, gain_ref, shift_ref, count):
    totals = jnp.sum(sums_ref[...], axis=0)
    lane = lax.broadcasted_iota(jnp.int32, totals.shape, 1)
    for width in (1, 2):
        back = pltpu.roll(totals, width, 1)
        ahead = pltpu.roll(totals, totals.shape[1] - width, 1)
        totals = totals + jnp.where(lane // width % 2 == 0, ahead, back)
    totals = totals * (1.0 / count)
    mean = totals[0:1]
    var = totals[1:2] - mean * mean
    scale = gain_ref[...] / jnp.sqrt(var + EPS)
    return 0.5 * scale, 0.5 * (shift_ref[...] - mean * scale)


def silu_of_double(half):
    return half + half * jnp.tanh(half)


def edges():
    th = lax.axis_index("th_0") * lax.axis_size("th_1") + lax.axis_index("th_1")
    tw = lax.axis_index("tw_0") * lax.axis_size("tw_1") + lax.axis_index("tw_1")
    section = lax.axis_index("section")
    last_th = lax.axis_size(TH) - 1
    last_tw = lax.axis_size(TW) - 1
    tests = (section > 0, th > 0, th < last_th, tw > 0, tw < last_tw)
    return [jnp.where(t, 1.0, 0.0).astype(F32) for t in tests]


def store_act(act_ref, h, m, pairs, row_ok, before_ok, column_ok):
    ok = row_ok if column_ok is None else row_ok * column_ok
    pairs = [pairs[0] * (ok * before_ok), pairs[1] * ok, pairs[2] * ok]
    low = lax.broadcasted_iota(jnp.int32, pairs[0].shape, 0) < 4
    mid = [pltpu.roll(jnp.where(low, b, a), 4, 0) for a, b in zip(pairs[:2], pairs[1:])]
    for dt, halves in enumerate((pairs[:2], mid, pairs[1:])):
        act_ref[dt, h, m] = jnp.concatenate(halves, 0).astype(BF16)


def column_masks(left_ok, right_ok):
    chunk = lax.broadcasted_iota(jnp.int32, (8, 128), 0) % 4
    return jnp.where(chunk == 0, left_ok, 1.0), jnp.where(chunk == 3, right_ok, 1.0)


def conv_block(act_ref, kernel_ref, pair_ref, rows_ref, single_ref, start, rows, cols):
    slabs = [(dt, di) for dt in range(3) for di in range(3)]

    def lhs(parts, width, height=rows):
        parts = [act_ref[dt, pl.ds(start + di, height), dj : dj + width] for dt, di, dj in parts]
        return jnp.concatenate([p.reshape(height * width * 16, 128) for p in parts], 1)

    def tap(dt, di, dj):
        k = ((dt * 3 + di) * 3 + dj) * 128
        return kernel_ref[k : k + 128, :]

    def wide(slab):
        return jnp.concatenate([tap(*slab, 0), tap(*slab, 1)], 1)

    for k in range(0, 9, 2):
        first = slabs[k]
        if k < 8:
            left = lhs([(*first, 0), (*slabs[k + 1], 0)], cols + 1)
            right = jnp.concatenate([wide(first), wide(slabs[k + 1])], 0)
        else:
            left = lhs([(*first, 0), (*first, 2)], cols + 1)
            last = tap(*first, 2)
            last = jnp.concatenate([last, jnp.zeros_like(last)], 1)
            right = jnp.concatenate([wide(first), last], 0)
        new = jnp.dot(left, right, preferred_element_type=F32)
        pair_ref[...] = new if k == 0 else pair_ref[...] + new
    for k, frames in enumerate(((0, 1), (2,))):
        left = lhs([(dt, 0, 2) for dt in frames], cols, rows + 1)
        right = jnp.concatenate(
            [jnp.concatenate([tap(dt, 0, 2), tap(dt, 1, 2)], 1) for dt in frames], 0
        )
        new = jnp.dot(left, right, preferred_element_type=F32)
        rows_ref[...] = new if k == 0 else rows_ref[...] + new
    left = lhs([(0, 2, 2), (1, 2, 2)], cols)
    right = jnp.concatenate([tap(0, 2, 2), tap(1, 2, 2)], 0)
    single_ref[...] = jnp.dot(left, right, preferred_element_type=F32)


def clear_last_column(act_ref, rows, column):
    for h in range(rows):
        act_ref[2, h, column] = jnp.zeros((16, 128), BF16)


def prepare_body(feat_ref, last_ref, top_ref, bottom_ref, head_ref, tail_ref, sums_ref):
    last_ref[...] = feat_ref[2:4]
    top_ref[...] = feat_ref[:, 0:2]
    bottom_ref[...] = feat_ref[:, 14:16]
    head_ref[...] = feat_ref[:, :, 0:2]
    tail_ref[...] = feat_ref[:, :, 30:32]
    first = jnp.zeros((8, 128), F32)
    second = jnp.zeros((8, 128), F32)
    for t in range(4):
        for h in range(0, 16, 4):
            part = feat_ref[t, h : h + 4].astype(F32).reshape(16, 8, 128)
            first += jnp.sum(part, 0)
            second += jnp.sum(part * part, 0)
    sums_ref[0:1, :] = jnp.sum(first, 0, keepdims=True)
    sums_ref[1:2, :] = jnp.sum(second, 0, keepdims=True)


ROWS1, COLS1, BLOCK1 = 18, CHUNK + 2, 18
ROWS2, COLS2, BLOCK2 = 16, CHUNK, 16


def first_body(count, feat_ref, before_ref, above_ref, below_ref, left_ref, right_ref, sums_ref,
               gain_ref, shift_ref, kernel_ref, hidden_ref, halo_ref, out_sums_ref,
               flat_ref, act_ref, pair_ref, rows_ref, single_ref, taps_ref, taps_sem):
    fetch = pltpu.make_async_copy(kernel_ref, taps_ref, taps_sem)
    fetch.start()
    scale, offset = scale_and_offset(sums_ref, gain_ref, shift_ref, count)
    before_ok, above_ok, below_ok, left_ok, right_ok = edges()
    left_mask, right_mask = column_masks(left_ok, right_ok)

    flat_ref[2:6, 2:18, 8:40] = feat_ref[...].astype(F32)
    flat_ref[0:2, 2:18, 8:40] = before_ref[...].astype(F32)
    flat_ref[:, 0:2, 8:40] = above_ref[...].astype(F32)
    flat_ref[:, 18:20, 8:40] = below_ref[...].astype(F32)
    flat_ref[:, :, 6:8] = left_ref[...].astype(F32)
    flat_ref[:, :, 40:42] = right_ref[...].astype(F32)

    def fill(h, _):
        row_ok = jnp.where(h < 2, above_ok, jnp.where(h >= 18, below_ok, 1.0))
        for m in range(COLS1 + 2):
            pairs = []
            for t in (0, 2, 4):
                raw = jnp.concatenate(
                    [flat_ref[t + i, h, pl.ds(6 + m, 4, stride=8), :] for i in range(2)], 0
                )
                pairs.append(silu_of_double(raw * scale + offset))
            column_ok = left_mask if m < 2 else right_mask if m >= COLS1 else None
            store_act(act_ref, h, m, pairs, row_ok, before_ok, column_ok)
        return 0

    lax.fori_loop(0, ROWS1 + 2, fill, 0)

    clear_last_column(act_ref, ROWS1 + 2, COLS1 + 2)
    fetch.wait()

    def conv(b, _):
        conv_block(act_ref, taps_ref, pair_ref, rows_ref, single_ref, b * BLOCK1, BLOCK1, COLS1)
        both = pair_ref[...].reshape(BLOCK1, COLS1 + 1, 16, 256)
        total = both[:, :COLS1, :, :128] + both[:, 1:, :, 128:]
        both = rows_ref[...].reshape(BLOCK1 + 1, COLS1, 16, 256)
        total += both[:BLOCK1, :, :, :128] + both[1:, :, :, 128:]
        total += single_ref[...].reshape(BLOCK1, COLS1, 16, 128)
        hidden_ref[pl.ds(b * BLOCK1, BLOCK1)] = total
        return 0

    lax.fori_loop(0, ROWS1 // BLOCK1, conv, 0)

    def total(h, carry):
        own = hidden_ref[h, 1 : CHUNK + 1].reshape(CHUNK * 2, 8, 128)
        return carry[0] + jnp.sum(own, 0), carry[1] + jnp.sum(own * own, 0)

    zero = jnp.zeros((8, 128), F32)
    first, second = lax.fori_loop(1, ROWS1 - 1, total, (zero, zero))
    out_sums_ref[0:1, :] = jnp.sum(first, 0, keepdims=True)
    out_sums_ref[1:2, :] = jnp.sum(second, 0, keepdims=True)

    def last_frames(h, _):
        for j in range(COLS1 // 2):
            both = [hidden_ref[h, 2 * j + i, 8:16, :] for i in range(2)]
            halo_ref[h, j] = jnp.concatenate(both, 0).astype(BF16)
        return 0

    lax.fori_loop(0, ROWS1, last_frames, 0)


def second_body(count, hidden_ref, halo_ref, sums_ref, gain_ref, shift_ref, kernel_ref, feat_ref,
                out_ref, act_ref, pair_ref, rows_ref, single_ref, flat_ref):
    scale, offset = scale_and_offset(sums_ref, gain_ref, shift_ref, count)
    before_ok, above_ok, below_ok, left_ok, right_ok = edges()
    left_mask, right_mask = column_masks(left_ok, right_ok)

    def fill(h, _):
        row_ok = jnp.where(h < 1, above_ok, jnp.where(h >= 17, below_ok, 1.0))
        for m in range(COLS2 + 2):
            halo = halo_ref[h, m // 2].astype(F32)[m % 2 * 8 : m % 2 * 8 + 8]
            raws = (halo, hidden_ref[h, m, 0:8, :], hidden_ref[h, m, 8:16, :])
            pairs = [silu_of_double(raw * scale + offset) for raw in raws]
            column_ok = left_mask if m < 1 else right_mask if m > COLS2 else None
            store_act(act_ref, h, m, pairs, row_ok, before_ok, column_ok)
        return 0

    lax.fori_loop(0, ROWS2 + 2, fill, 0)

    clear_last_column(act_ref, ROWS2 + 2, COLS2 + 2)

    def conv(b, _):
        conv_block(act_ref, kernel_ref, pair_ref, rows_ref, single_ref, b * BLOCK2, BLOCK2, COLS2)

        def spread(i, _):
            h = b * BLOCK2 + i
            for m in range(COLS2):
                at = pl.multiple_of((i * (COLS2 + 1) + m) * 16, 16)
                tile = pair_ref[pl.ds(at, 16), :128] + pair_ref[pl.ds(at + 16, 16), 128:]
                at = pl.multiple_of((i * COLS2 + m) * 16, 16)
                below = pl.multiple_of(((i + 1) * COLS2 + m) * 16, 16)
                tile += rows_ref[pl.ds(at, 16), :128] + rows_ref[pl.ds(below, 16), 128:]
                tile += single_ref[pl.ds(at, 16), :]
                for t in range(4):
                    flat_ref[t, pl.ds(m, 4, stride=8), :] = tile[4 * t : 4 * t + 4]
            for t in range(4):
                total = feat_ref[t, h].astype(F32) + flat_ref[t]
                out_ref[t, h] = total.astype(BF16)
            return 0

        lax.fori_loop(0, BLOCK2, spread, 0)
        return 0

    lax.fori_loop(0, ROWS2 // BLOCK2, conv, 0)


def in_vmem(count):
    return [pl.BlockSpec(memory_space=pltpu.VMEM)] * count


def shards(features, norm_gain, norm_shift, first_kernel, second_gain, second_shift, second_kernel):
    count = features.size // features.shape[-1] * PER
    for axis in ("section", *TH, *TW):
        count *= lax.axis_size(axis)
    last, top, bottom, head, tail, sums = pl.pallas_call(
        prepare_body,
        out_shape=tuple(
            jax.ShapeDtypeStruct(shape, BF16)
            for shape in (
                (2, 16, 32, 128), (4, 2, 32, 128), (4, 2, 32, 128), (4, 16, 2, 128), (4, 16, 2, 128)
            )
        ) + (jax.ShapeDtypeStruct((2, 128), F32),),
        in_specs=in_vmem(1),
        out_specs=tuple(in_vmem(6)),
        compiler_params=pltpu.CompilerParams(vmem_limit_bytes=VMEM),
        name="prepare",
    )(features)

    before = shifted(last, "section", 1)
    sums = gathered_sum(sums, TW)
    before, sums = lax.optimization_barrier((before, sums))
    above, below = swapped(
        jnp.concatenate([before[:, -2:], bottom], 0),
        jnp.concatenate([before[:, :2], top], 0),
        TH,
        (lax.axis_index("th_1") & 1) == 1,
    )
    sums = gathered_sum(sums, "th_1")
    sums = gathered_sum(sums, "section")
    above, below, sums = lax.optimization_barrier((above, below, sums))

    def columns(own, s):
        own = jnp.concatenate([before[:, :, s], own], 0)
        return jnp.concatenate([above[:, :, s], own, below[:, :, s]], 1)

    left, right = swapped(
        columns(tail, slice(-2, None)),
        columns(head, slice(0, 2)),
        TW,
        lax.axis_index("tw_1") == 1,
    )
    sums = lax.all_gather(sums, "th_0")

    hidden, halo, sums = pl.pallas_call(
        functools.partial(first_body, count),
        out_shape=(
            jax.ShapeDtypeStruct((ROWS1, COLS1, 16, 128), F32),
            pltpu.VMEM((ROWS1, COLS1 // 2, 16, 128), BF16),
            jax.ShapeDtypeStruct((2, 128), F32),
        ),
        in_specs=[*in_vmem(9), pl.BlockSpec(memory_space=pltpu.HBM)],
        out_specs=tuple(in_vmem(3)),
        scratch_shapes=[
            pltpu.VMEM((6, 20, 48, 128), F32),
            pltpu.VMEM((3, ROWS1 + 2, COLS1 + 3, 16, 128), BF16),
            pltpu.VMEM((BLOCK1 * (COLS1 + 1) * 16, 256), F32),
            pltpu.VMEM(((BLOCK1 + 1) * COLS1 * 16, 256), F32),
            pltpu.VMEM((BLOCK1 * COLS1 * 16, 128), F32),
            pltpu.VMEM((27 * 128, 128), BF16),
            pltpu.SemaphoreType.DMA,
        ],
        compiler_params=pltpu.CompilerParams(vmem_limit_bytes=VMEM),
        name="first_conv",
    )(features, before, above, below, left, right, sums, norm_gain[None], norm_shift[None],
      pltpu.with_memory_space_constraint(first_kernel.reshape(-1, 128), pltpu.HBM))

    halo = shifted(halo, "section", 1)
    for axis in (TW, "th_1", "section"):
        sums = gathered_sum(sums, axis)
    sums = lax.all_gather(sums, "th_0")

    return pl.pallas_call(
        functools.partial(second_body, count),
        out_shape=jax.ShapeDtypeStruct(features.shape, BF16),
        in_specs=in_vmem(7),
        out_specs=in_vmem(1)[0],
        scratch_shapes=[
            pltpu.VMEM((3, ROWS2 + 2, COLS2 + 3, 16, 128), BF16),
            pltpu.VMEM((BLOCK2 * (COLS2 + 1) * 16, 256), F32),
            pltpu.VMEM(((BLOCK2 + 1) * COLS2 * 16, 256), F32),
            pltpu.VMEM((BLOCK2 * COLS2 * 16, 128), F32),
            pltpu.VMEM((4, 32, 128), F32),
        ],
        compiler_params=pltpu.CompilerParams(vmem_limit_bytes=VMEM),
        name="second_conv",
    )(hidden, halo, sums, second_gain[None], second_shift[None], second_kernel.reshape(-1, 128), features)


def solution(mesh):
    torus = Mesh(
        mesh.devices.reshape(mesh.shape["section"], 4, 4, 4, 2),
        ("section", "th_0", "th_1", "tw_0", "tw_1"),
    )
    return jax.shard_map(
        shards,
        mesh=torus,
        in_specs=(P("section", TH, TW, None), P(), P(), P(), P(), P(), P()),
        out_specs=P("section", TH, TW, None),
        check_vma=False,
    )
```

```python
import functools

import jax
import jax.numpy as jnp
from jax import lax
from jax.experimental import pallas as pl
from jax.experimental.pallas import tpu as pltpu
from jax.sharding import Mesh
from jax.sharding import PartitionSpec as P

TH = ("th_0", "th_1")
TW = ("tw_0", "tw_1")
PER = 4
CHUNK = 8
EPS = 1e-06
VMEM = 20 * 2**20
F32 = jnp.float32
BF16 = jnp.bfloat16


def gathered_sum(value, axis):
    return jnp.sum(lax.all_gather(value, axis), axis=0)


def shifted(value, axis, step):
    count = lax.axis_size(axis)
    pairs = [(i, i + step) for i in range(count) if 0 <= i + step < count]
    return lax.ppermute(value, axis, pairs)


def swapped(toward_next, toward_last, axis, odd):
    count = lax.axis_size(axis)

    def swap(value, first):
        pairs = [(i, i + 1) for i in range(first, count - 1, 2)]
        return lax.ppermute(value, axis, pairs + [(b, a) for a, b in pairs])

    even_first = swap(jnp.where(odd, toward_last, toward_next), 0)
    odd_first = swap(jnp.where(odd, toward_next, toward_last), 1)
    return jnp.where(odd, even_first, odd_first), jnp.where(odd, odd_first, even_first)


def scale_and_offset(sums_ref, gain_ref, shift_ref, count):
    totals = jnp.sum(sums_ref[...], axis=0)
    lane = lax.broadcasted_iota(jnp.int32, totals.shape, 1)
    for width in (1, 2):
        back = pltpu.roll(totals, width, 1)
        ahead = pltpu.roll(totals, totals.shape[1] - width, 1)
        totals = totals + jnp.where(lane // width % 2 == 0, ahead, back)
    totals = totals * (1.0 / count)
    mean = totals[0:1]
    var = totals[1:2] - mean * mean
    scale = gain_ref[...] / jnp.sqrt(var + EPS)
    return 0.5 * scale, 0.5 * (shift_ref[...] - mean * scale)


def silu_of_double(half):
    return half + half * jnp.tanh(half)


def edges():
    th = lax.axis_index("th_0") * lax.axis_size("th_1") + lax.axis_index("th_1")
    tw = lax.axis_index("tw_0") * lax.axis_size("tw_1") + lax.axis_index("tw_1")
    section = lax.axis_index("section")
    last_th = lax.axis_size(TH) - 1
    last_tw = lax.axis_size(TW) - 1
    tests = (section > 0, th > 0, th < last_th, tw > 0, tw < last_tw)
    return [jnp.where(t, 1.0, 0.0).astype(F32) for t in tests]


def store_act(act_ref, h, m, pairs, row_ok, before_ok, column_ok):
    ok = row_ok if column_ok is None else row_ok * column_ok
    pairs = [pairs[0] * (ok * before_ok), pairs[1] * ok, pairs[2] * ok]
    low = lax.broadcasted_iota(jnp.int32, pairs[0].shape, 0) < 4
    mid = [pltpu.roll(jnp.where(low, b, a), 4, 0) for a, b in zip(pairs[:2], pairs[1:])]
    for dt, halves in enumerate((pairs[:2], mid, pairs[1:])):
        act_ref[dt, h, m] = jnp.concatenate(halves, 0).astype(BF16)


def column_masks(left_ok, right_ok):
    chunk = lax.broadcasted_iota(jnp.int32, (8, 128), 0) % 4
    return jnp.where(chunk == 0, left_ok, 1.0), jnp.where(chunk == 3, right_ok, 1.0)


def conv_block(act_ref, kernel_ref, pair_ref, rows_ref, single_ref, start, rows, cols):
    slabs = [(dt, di) for dt in range(3) for di in range(3)]

    def lhs(parts, width, height=rows):
        parts = [act_ref[dt, pl.ds(start + di, height), dj : dj + width] for dt, di, dj in parts]
        return jnp.concatenate([p.reshape(height * width * 16, 128) for p in parts], 1)

    def tap(dt, di, dj):
        k = ((dt * 3 + di) * 3 + dj) * 128
        return kernel_ref[k : k + 128, :]

    def wide(slab):
        return jnp.concatenate([tap(*slab, 0), tap(*slab, 1)], 1)

    for k in range(0, 9, 2):
        first = slabs[k]
        if k < 8:
            left = lhs([(*first, 0), (*slabs[k + 1], 0)], cols + 1)
            right = jnp.concatenate([wide(first), wide(slabs[k + 1])], 0)
        else:
            left = lhs([(*first, 0), (*first, 2)], cols + 1)
            last = tap(*first, 2)
            last = jnp.concatenate([last, jnp.zeros_like(last)], 1)
            right = jnp.concatenate([wide(first), last], 0)
        new = jnp.dot(left, right, preferred_element_type=F32)
        pair_ref[...] = new if k == 0 else pair_ref[...] + new
    for k, frames in enumerate(((0, 1), (2,))):
        left = lhs([(dt, 0, 2) for dt in frames], cols, rows + 1)
        right = jnp.concatenate(
            [jnp.concatenate([tap(dt, 0, 2), tap(dt, 1, 2)], 1) for dt in frames], 0
        )
        new = jnp.dot(left, right, preferred_element_type=F32)
        rows_ref[...] = new if k == 0 else rows_ref[...] + new
    left = lhs([(0, 2, 2), (1, 2, 2)], cols)
    right = jnp.concatenate([tap(0, 2, 2), tap(1, 2, 2)], 0)
    single_ref[...] = jnp.dot(left, right, preferred_element_type=F32)


def clear_last_column(act_ref, rows, column):
    for h in range(rows):
        act_ref[2, h, column] = jnp.zeros((16, 128), BF16)


def prepare_body(feat_ref, last_ref, top_ref, bottom_ref, head_ref, tail_ref, sums_ref):
    last_ref[...] = feat_ref[2:4]
    top_ref[...] = feat_ref[:, 0:2]
    bottom_ref[...] = feat_ref[:, 14:16]
    head_ref[...] = feat_ref[:, :, 0:2]
    tail_ref[...] = feat_ref[:, :, 30:32]
    first = jnp.zeros((8, 128), F32)
    second = jnp.zeros((8, 128), F32)
    for t in range(4):
        for h in range(0, 16, 4):
            part = feat_ref[t, h : h + 4].astype(F32).reshape(16, 8, 128)
            first += jnp.sum(part, 0)
            second += jnp.sum(part * part, 0)
    sums_ref[0:1, :] = jnp.sum(first, 0, keepdims=True)
    sums_ref[1:2, :] = jnp.sum(second, 0, keepdims=True)


ROWS1, COLS1, BLOCK1 = 18, CHUNK + 2, 18
ROWS2, COLS2, BLOCK2 = 16, CHUNK, 16


def first_body(count, feat_ref, before_ref, above_ref, below_ref, left_ref, right_ref, sums_ref,
               gain_ref, shift_ref, kernel_ref, hidden_ref, halo_ref, out_sums_ref,
               flat_ref, act_ref, pair_ref, rows_ref, single_ref, taps_ref, taps_sem):
    fetch = pltpu.make_async_copy(kernel_ref, taps_ref, taps_sem)
    fetch.start()
    scale, offset = scale_and_offset(sums_ref, gain_ref, shift_ref, count)
    before_ok, above_ok, below_ok, left_ok, right_ok = edges()
    left_mask, right_mask = column_masks(left_ok, right_ok)

    flat_ref[2:6, 2:18, 8:40] = feat_ref[...].astype(F32)
    flat_ref[0:2, 2:18, 8:40] = before_ref[...].astype(F32)
    flat_ref[:, 0:2, 8:40] = above_ref[...].astype(F32)
    flat_ref[:, 18:20, 8:40] = below_ref[...].astype(F32)
    flat_ref[:, :, 6:8] = left_ref[...].astype(F32)
    flat_ref[:, :, 40:42] = right_ref[...].astype(F32)

    def fill(h, _):
        row_ok = jnp.where(h < 2, above_ok, jnp.where(h >= 18, below_ok, 1.0))
        for m in range(COLS1 + 2):
            pairs = []
            for t in (0, 2, 4):
                raw = jnp.concatenate(
                    [flat_ref[t + i, h, pl.ds(6 + m, 4, stride=8), :] for i in range(2)], 0
                )
                pairs.append(silu_of_double(raw * scale + offset))
            column_ok = left_mask if m < 2 else right_mask if m >= COLS1 else None
            store_act(act_ref, h, m, pairs, row_ok, before_ok, column_ok)
        return 0

    lax.fori_loop(0, ROWS1 + 2, fill, 0, unroll=2)

    clear_last_column(act_ref, ROWS1 + 2, COLS1 + 2)
    fetch.wait()

    def conv(b, _):
        conv_block(act_ref, taps_ref, pair_ref, rows_ref, single_ref, b * BLOCK1, BLOCK1, COLS1)
        both = pair_ref[...].reshape(BLOCK1, COLS1 + 1, 16, 256)
        total = both[:, :COLS1, :, :128] + both[:, 1:, :, 128:]
        both = rows_ref[...].reshape(BLOCK1 + 1, COLS1, 16, 256)
        total += both[:BLOCK1, :, :, :128] + both[1:, :, :, 128:]
        total += single_ref[...].reshape(BLOCK1, COLS1, 16, 128)
        hidden_ref[pl.ds(b * BLOCK1, BLOCK1)] = total
        return 0

    lax.fori_loop(0, ROWS1 // BLOCK1, conv, 0)

    def total(h, carry):
        own = hidden_ref[h, 1 : CHUNK + 1].reshape(CHUNK * 2, 8, 128)
        return carry[0] + jnp.sum(own, 0), carry[1] + jnp.sum(own * own, 0)

    zero = jnp.zeros((8, 128), F32)
    first, second = lax.fori_loop(1, ROWS1 - 1, total, (zero, zero), unroll=4)
    out_sums_ref[0:1, :] = jnp.sum(first, 0, keepdims=True)
    out_sums_ref[1:2, :] = jnp.sum(second, 0, keepdims=True)

    def last_frames(h, _):
        for j in range(COLS1 // 2):
            both = [hidden_ref[h, 2 * j + i, 8:16, :] for i in range(2)]
            halo_ref[h, j] = jnp.concatenate(both, 0).astype(BF16)
        return 0

    lax.fori_loop(0, ROWS1, last_frames, 0, unroll=3)


def second_body(count, hidden_ref, halo_ref, sums_ref, gain_ref, shift_ref, kernel_ref, feat_ref,
                out_ref, act_ref, pair_ref, rows_ref, single_ref, flat_ref):
    scale, offset = scale_and_offset(sums_ref, gain_ref, shift_ref, count)
    before_ok, above_ok, below_ok, left_ok, right_ok = edges()
    left_mask, right_mask = column_masks(left_ok, right_ok)

    def fill(h, _):
        row_ok = jnp.where(h < 1, above_ok, jnp.where(h >= 17, below_ok, 1.0))
        for m in range(COLS2 + 2):
            halo = halo_ref[h, m // 2].astype(F32)[m % 2 * 8 : m % 2 * 8 + 8]
            raws = (halo, hidden_ref[h, m, 0:8, :], hidden_ref[h, m, 8:16, :])
            pairs = [silu_of_double(raw * scale + offset) for raw in raws]
            column_ok = left_mask if m < 1 else right_mask if m > COLS2 else None
            store_act(act_ref, h, m, pairs, row_ok, before_ok, column_ok)
        return 0

    lax.fori_loop(0, ROWS2 + 2, fill, 0, unroll=2)

    clear_last_column(act_ref, ROWS2 + 2, COLS2 + 2)

    def conv(b, _):
        conv_block(act_ref, kernel_ref, pair_ref, rows_ref, single_ref, b * BLOCK2, BLOCK2, COLS2)

        def spread(i, _):
            h = b * BLOCK2 + i
            for m in range(COLS2):
                at = pl.multiple_of((i * (COLS2 + 1) + m) * 16, 16)
                tile = pair_ref[pl.ds(at, 16), :128] + pair_ref[pl.ds(at + 16, 16), 128:]
                at = pl.multiple_of((i * COLS2 + m) * 16, 16)
                below = pl.multiple_of(((i + 1) * COLS2 + m) * 16, 16)
                tile += rows_ref[pl.ds(at, 16), :128] + rows_ref[pl.ds(below, 16), 128:]
                tile += single_ref[pl.ds(at, 16), :]
                for t in range(4):
                    flat_ref[t, pl.ds(m, 4, stride=8), :] = tile[4 * t : 4 * t + 4]
            for t in range(4):
                total = feat_ref[t, h].astype(F32) + flat_ref[t]
                out_ref[t, h] = total.astype(BF16)
            return 0

        lax.fori_loop(0, BLOCK2, spread, 0, unroll=2)
        return 0

    lax.fori_loop(0, ROWS2 // BLOCK2, conv, 0)


def in_vmem(count):
    return [pl.BlockSpec(memory_space=pltpu.VMEM)] * count


def shards(features, norm_gain, norm_shift, first_kernel, second_gain, second_shift, second_kernel):
    count = features.size // features.shape[-1] * PER
    for axis in ("section", *TH, *TW):
        count *= lax.axis_size(axis)
    last, top, bottom, head, tail, sums = pl.pallas_call(
        prepare_body,
        out_shape=tuple(
            jax.ShapeDtypeStruct(shape, BF16)
            for shape in (
                (2, 16, 32, 128), (4, 2, 32, 128), (4, 2, 32, 128), (4, 16, 2, 128), (4, 16, 2, 128)
            )
        ) + (jax.ShapeDtypeStruct((2, 128), F32),),
        in_specs=in_vmem(1),
        out_specs=tuple(in_vmem(6)),
        compiler_params=pltpu.CompilerParams(vmem_limit_bytes=VMEM),
        name="prepare",
    )(features)

    before = shifted(last, "section", 1)
    sums = gathered_sum(sums, TW)
    before, sums = lax.optimization_barrier((before, sums))
    above, below = swapped(
        jnp.concatenate([before[:, -2:], bottom], 0),
        jnp.concatenate([before[:, :2], top], 0),
        TH,
        (lax.axis_index("th_1") & 1) == 1,
    )
    sums = gathered_sum(sums, "th_1")
    sums = gathered_sum(sums, "section")
    above, below, sums = lax.optimization_barrier((above, below, sums))

    def columns(own, s):
        own = jnp.concatenate([before[:, :, s], own], 0)
        return jnp.concatenate([above[:, :, s], own, below[:, :, s]], 1)

    left, right = swapped(
        columns(tail, slice(-2, None)),
        columns(head, slice(0, 2)),
        TW,
        lax.axis_index("tw_1") == 1,
    )
    sums = lax.all_gather(sums, "th_0")

    hidden, halo, sums = pl.pallas_call(
        functools.partial(first_body, count),
        out_shape=(
            jax.ShapeDtypeStruct((ROWS1, COLS1, 16, 128), F32),
            pltpu.VMEM((ROWS1, COLS1 // 2, 16, 128), BF16),
            jax.ShapeDtypeStruct((2, 128), F32),
        ),
        in_specs=[*in_vmem(9), pl.BlockSpec(memory_space=pltpu.HBM)],
        out_specs=tuple(in_vmem(3)),
        scratch_shapes=[
            pltpu.VMEM((6, 20, 48, 128), F32),
            pltpu.VMEM((3, ROWS1 + 2, COLS1 + 3, 16, 128), BF16),
            pltpu.VMEM((BLOCK1 * (COLS1 + 1) * 16, 256), F32),
            pltpu.VMEM(((BLOCK1 + 1) * COLS1 * 16, 256), F32),
            pltpu.VMEM((BLOCK1 * COLS1 * 16, 128), F32),
            pltpu.VMEM((27 * 128, 128), BF16),
            pltpu.SemaphoreType.DMA,
        ],
        compiler_params=pltpu.CompilerParams(vmem_limit_bytes=VMEM),
        name="first_conv",
    )(features, before, above, below, left, right, sums, norm_gain[None], norm_shift[None],
      pltpu.with_memory_space_constraint(first_kernel.reshape(-1, 128), pltpu.HBM))

    halo = shifted(halo, "section", 1)
    for axis in (TW, "th_1", "section"):
        sums = gathered_sum(sums, axis)
    sums = lax.all_gather(sums, "th_0")

    return pl.pallas_call(
        functools.partial(second_body, count),
        out_shape=jax.ShapeDtypeStruct(features.shape, BF16),
        in_specs=in_vmem(7),
        out_specs=in_vmem(1)[0],
        scratch_shapes=[
            pltpu.VMEM((3, ROWS2 + 2, COLS2 + 3, 16, 128), BF16),
            pltpu.VMEM((BLOCK2 * (COLS2 + 1) * 16, 256), F32),
            pltpu.VMEM(((BLOCK2 + 1) * COLS2 * 16, 256), F32),
            pltpu.VMEM((BLOCK2 * COLS2 * 16, 128), F32),
            pltpu.VMEM((4, 32, 128), F32),
        ],
        compiler_params=pltpu.CompilerParams(vmem_limit_bytes=VMEM),
        name="second_conv",
    )(hidden, halo, sums, second_gain[None], second_shift[None], second_kernel.reshape(-1, 128), features)


def solution(mesh):
    torus = Mesh(
        mesh.devices.reshape(mesh.shape["section"], 4, 4, 4, 2),
        ("section", "th_0", "th_1", "tw_0", "tw_1"),
    )
    return jax.shard_map(
        shards,
        mesh=torus,
        in_specs=(P("section", TH, TW, None), P(), P(), P(), P(), P(), P()),
        out_specs=P("section", TH, TW, None),
        check_vma=False,
    )
```
